256 devices in a mesh: cohort: 8 (over z_lo, core), gene: 32 (over x, y, z_hi).
Axes of the slice: x: 4, y: 4, z: 8 (z_hi: 2, z_lo: 4; z = z_hi * 4 + z_lo), core: 2. Of those that a mesh axis runs over, the one named last changes fastest.
Arguments:
- expression: bfloat16 [24000, 3200], P('gene'), as said below
- sample_index: int32 [8, 400], P('cohort'), may hold values from 0 to 3199, as said below
- gene_block: int32 [24000], P('gene'), may hold values from 0 to 127
Outputs:
- connectivity: float32 [4864, 128], P(('cohort', 'gene'))
The draws below stay inside these ranges and needn't reach their ends.
Inputs may be any that keep to these rules, and one draw needn't show every extreme that they name: `sample_index`: the entries together are a permutation of the 3200 pooled samples, 400 in each cohort. Finite expression values; genes of a module co-vary with a strength that differs between cohorts.
All inputs are finite; a program needn't handle non-finite values.
Results may differ from the reference program's by a relative error of at most 0.00097.
Values may be sent and summed in bfloat16 or wider, within the bound.
No kernel may reach another device: no remote copies, remote signals or barrier semaphores. Data moves between devices by JAX's collectives and lax.ppermute only.
A program may use at most 64 MiB of HBM per device.

```python
import jax
import jax.numpy as jnp
from jax import lax

G = 24000
S = 400
MODULES = 128
ROW_DEV = 152
COHORTS = 8
N_GENE = 32


def shared_labels(key):
    order = jax.random.permutation(jax.random.fold_in(key, 11), COHORTS * S).astype(jnp.int32)
    labels = jax.random.randint(jax.random.fold_in(key, 12), (G,), 0, MODULES).astype(jnp.int32)
    return (order, labels)


def draw_sample_index(key, part):
    order, labels = shared_labels(key)
    return order.reshape(COHORTS, S)


def draw_gene_block(key, part):
    order, labels = shared_labels(key)
    return labels


def draw_expression(key, part):
    order, labels = shared_labels(key)
    owner = (jnp.argsort(order) // S).astype(jnp.int32)
    strength = jax.random.uniform(jax.random.fold_in(key, 21), (COHORTS, MODULES), jnp.float32, 0.5, 3.0)
    loading = jax.random.uniform(jax.random.fold_in(key, 22), (G,), jnp.float32, 0.5, 1.5)
    factor = jax.random.normal(jax.random.fold_in(key, 23), (MODULES, COHORTS * S), jnp.float32)
    pooled_strength = jnp.take(strength, owner, axis=0)
    gene_strength = jnp.take(pooled_strength, labels, axis=1).T
    signal = loading[:, None] * gene_strength * jnp.take(factor, labels, axis=0)
    noise = jax.random.normal(jax.random.fold_in(key, 24), (G, COHORTS * S), jnp.float32)
    values = signal + noise
    return values.astype(jnp.bfloat16)


def setup_inputs(seed: int = 0) -> dict:
    splits = jax.random.split(jax.random.key(seed), 4)
    return {
        "expression": draw_expression(jax.random.fold_in(splits[3], 71), 0),
        "sample_index": draw_sample_index(jax.random.fold_in(splits[3], 71), 0),
        "gene_block": draw_gene_block(jax.random.fold_in(splits[3], 71), 0),
    }


def standardize(block):
    values = block.astype(jnp.float32)
    centred = values - lax.optimization_barrier(jnp.mean(values, axis=1, keepdims=True))
    spread = jnp.sqrt(lax.optimization_barrier(jnp.sum(centred * centred, axis=1, keepdims=True)) + 0.01 * centred.shape[1])
    return (centred / spread).astype(jnp.bfloat16)

def power_twelve(corr):
    base = (1.0 + corr) * 0.5
    square = base * base
    fourth = square * square
    return (fourth * fourth * fourth).astype(jnp.bfloat16)

def reference(expression, sample_index, gene_block):
    per_block = G // N_GENE
    rows = jnp.arange(ROW_DEV * N_GENE, dtype=jnp.int32)
    window = rows // ROW_DEV * per_block + rows % ROW_DEV
    consensus = None
    for cohort in range(COHORTS):
        scores = standardize(jnp.take(expression, sample_index[cohort], axis=1))
        window_scores = jnp.take(scores, window, axis=0)
        corr = jnp.dot(scores.astype(jnp.float32), window_scores.astype(jnp.float32).T)
        adjacency = power_twelve(corr)
        consensus = adjacency if consensus is None else jnp.minimum(consensus, adjacency)
    onehot = (gene_block[:, None] == jnp.arange(MODULES, dtype=jnp.int32)[None, :]).astype(jnp.float32)
    degree = jnp.dot(consensus.astype(jnp.float32).T, onehot)
    return jnp.log1p(degree)
```

```python
import functools

import jax
import jax.numpy as jnp
from jax import lax
from jax.experimental import pallas as pl
from jax.experimental.pallas import tpu as pltpu
from jax.sharding import Mesh
from jax.sharding import PartitionSpec as P

MODULES = 128
ROW_DEV = 152
COHORTS = 8
SAMPLES = 400
POOL = COHORTS * SAMPLES
GENES = 750
ROWS = 19
LANES = 128
TILES = POOL // LANES
DEPTH = 512
PITCH = POOL + 4
GENE_BLOCKS = 6
COHORT_AXES = ("z_lo", "core")
GENE_AXES = ("x", "y", "z_hi")
ALL_AXES = COHORT_AXES + GENE_AXES
UNROLL = 32
F32 = jnp.float32
BF16 = jnp.bfloat16


def transpose_in(load, blocks, turned):
    def column(k, _):
        lane = pl.multiple_of(k * LANES, LANES)
        for b in range(blocks):
            tile = load(b, lane)
            turned[pl.ds(b * PITCH + lane, LANES), :] = tile.T
        return _

    lax.fori_loop(0, TILES, column, 0)


def gather_rows(order, turned, grouped, blocks):
    def some(i, _):
        first = i * UNROLL
        for u in range(UNROLL):
            sample = order[first + u]
            grouped[pl.ds(first + u, blocks, stride=PITCH), :] = turned[
                pl.ds(sample, blocks, stride=PITCH), :
            ]
        return _

    lax.fori_loop(0, POOL // UNROLL, some, 0)


def standardized(grouped, cohort, block):
    x = grouped[pl.ds(block * PITCH + cohort * SAMPLES, SAMPLES), :]
    centred = x - jnp.sum(x, axis=0, keepdims=True) * (1.0 / SAMPLES)
    spread = jnp.sqrt(jnp.sum(centred * centred, axis=0, keepdims=True) + 0.01 * SAMPLES)
    return centred * (1.0 / spread)


def gene_kernel(order, x_ref, z_ref, turned, grouped):
    def load(b, lane):
        rows = min(LANES, GENES - b * LANES)
        tile = x_ref[b * LANES : b * LANES + rows, pl.ds(lane, LANES)].astype(F32)
        if rows < LANES:
            tile = jnp.concatenate([tile, jnp.zeros((LANES - rows, LANES), F32)], axis=0)
        return tile

    transpose_in(load, GENE_BLOCKS, turned)
    gather_rows(order, turned, grouped, GENE_BLOCKS)

    def cohort(c, _):
        for b in range(GENE_BLOCKS):
            z = standardized(grouped, c, b)
            z = jnp.concatenate([z, jnp.zeros((DEPTH - SAMPLES, LANES), F32)], axis=0)
            z_ref[c, b * LANES : (b + 1) * LANES, :] = z.T.astype(BF16)
        return _

    lax.fori_loop(0, COHORTS, cohort, 0)


def genes(order, x):
    return pl.pallas_call(
        gene_kernel,
        out_shape=jax.ShapeDtypeStruct((COHORTS, GENE_BLOCKS * LANES, DEPTH), BF16),
        in_specs=[
            pl.BlockSpec(memory_space=pltpu.SMEM),
            pl.BlockSpec(memory_space=pltpu.VMEM),
        ],
        out_specs=pl.BlockSpec(memory_space=pltpu.VMEM),
        scratch_shapes=[
            pltpu.VMEM((GENE_BLOCKS * PITCH, LANES), F32),
            pltpu.VMEM((GENE_BLOCKS * PITCH, LANES), F32),
        ],
        compiler_params=pltpu.CompilerParams(vmem_limit_bytes=56 * 2**20),
        name="genes",
    )(order, x)


def window_kernel(units, rows, order, place, module_ref, z_ref, *refs):
    parts, (out_ref, turned, grouped, zw, low, consensus) = refs[:units], refs[units:]
    total = sum(len_of(p) for p in parts) * rows
    blocks = total // LANES
    strips = [(p, j, r) for p in parts for j in range(p.shape[0]) for r in range(0, rows, 8)]

    def load(b, lane):
        return jnp.concatenate(
            [p[j, r : r + 8, pl.ds(lane, LANES)].astype(F32) for p, j, r in strips[b * 16 : (b + 1) * 16]],
            axis=0,
        )

    transpose_in(load, blocks, turned)
    gather_rows(order, turned, grouped, blocks)

    low[...] = jnp.full(low.shape, 2.0, F32)
    zw[SAMPLES:, :] = jnp.zeros((DEPTH - SAMPLES, total), BF16)

    def cohort(c, _):
        for b in range(blocks):
            zw[:SAMPLES, b * LANES : (b + 1) * LANES] = standardized(grouped, c, b).astype(BF16)
        corr = jnp.dot(z_ref[c], zw[...], preferred_element_type=F32)
        low[...] = jnp.minimum(low[...], corr)
        return _

    lax.fori_loop(0, COHORTS, cohort, 0)

    base = (1.0 + jnp.maximum(low[...], -1.0)) * 0.5
    square = base * base
    fourth = square * square
    consensus[...] = (fourth * fourth * fourth).astype(BF16)
    module = lax.broadcasted_iota(jnp.int32, (MODULES, GENE_BLOCKS * LANES), 0)
    onehot = jnp.where(module_ref[...] == module, 1.0, 0.0).astype(BF16)
    degree = jnp.dot(onehot, consensus[...], preferred_element_type=F32)
    turned_degree = degree.T
    for i in range(total // rows):
        at = pl.multiple_of(place[i] * rows, 8)
        out_ref[pl.ds(at, rows), :] = turned_degree[i * rows : (i + 1) * rows, :]


def len_of(ref):
    return ref.shape[0]


def windows(order, place, module, z, parts):
    rows = parts[0].shape[1]
    count = sum(p.shape[0] for p in parts)
    total = count * rows
    blocks = total // LANES
    return pl.pallas_call(
        functools.partial(window_kernel, len(parts), rows),
        out_shape=jax.ShapeDtypeStruct((total, MODULES), F32),
        in_specs=[
            pl.BlockSpec(memory_space=pltpu.SMEM),
            pl.BlockSpec(memory_space=pltpu.SMEM),
        ]
        + [pl.BlockSpec(memory_space=pltpu.VMEM)] * (2 + len(parts)),
        out_specs=pl.BlockSpec(memory_space=pltpu.VMEM),
        scratch_shapes=[
            pltpu.VMEM((blocks * PITCH, LANES), F32),
            pltpu.VMEM((blocks * PITCH, LANES), F32),
            pltpu.VMEM((DEPTH, total), BF16),
            pltpu.VMEM((GENE_BLOCKS * LANES, total), F32),
            pltpu.VMEM((GENE_BLOCKS * LANES, total), BF16),
        ],
        compiler_params=pltpu.CompilerParams(vmem_limit_bytes=56 * 2**20),
        name=f"windows_{total}",
    )(order, place, module, z, *parts)


def shifted(array, axis, by):
    n = lax.axis_size(axis)
    return lax.ppermute(array, axis, [(i, (i + by) % n) for i in range(n)])


def gathered(unit, first, second):
    line = [unit] + [shifted(unit, first, by) for by in (1, 3, 2)]
    stack = jnp.stack(line)
    ahead, behind = shifted(stack, second, 1), shifted(stack, second, 3)
    far = [shifted(ahead[:2], second, 1), shifted(behind[2:], second, 3)]
    parts = [stack, ahead, behind, *far]
    one = (0, -1, 1, 2)
    where = [(a, 0) for a in one] + [(a, -1) for a in one] + [(a, 1) for a in one] + [(a, 2) for a in one]
    return parts, where


def places(where, first, second):
    spots = []
    for a, b in where:
        at = {first: (lax.axis_index(first) + a) % 4, second: (lax.axis_index(second) + b) % 4}
        spots.append(at["x"] * 4 + at["y"])
    return jnp.stack(spots).astype(jnp.int32)


def on_device(expression, sample_index, gene_block):
    z_lo, core = lax.axis_index("z_lo"), lax.axis_index("core")
    share = z_lo * 2 + core
    mirror = (3 - z_lo) * 2 + core
    own = lax.dynamic_slice(expression, (share * ROWS, 0), (ROWS, POOL))
    theirs = lax.dynamic_slice(expression, (mirror * ROWS, 0), (ROWS, POOL))
    pairs = [(z * 2 + h, (3 - z) * 2 + 1 - h) for z in range(4) for h in range(2)]
    across = lax.ppermute(theirs, ("z_lo", "z_hi"), pairs)

    both = jnp.concatenate([sample_index, lax.ppermute(sample_index, "core", [(0, 1), (1, 0)])])
    order = jnp.concatenate([both] + [shifted(both, "z_lo", by) for by in (1, 2, 3)]).reshape(POOL)

    near, near_at = gathered(own[:16], "x", "y")
    rest = jnp.concatenate([own[16:], across, jnp.zeros((2, POOL), BF16)])
    z = genes(order, expression)
    module = jnp.pad(gene_block, (0, GENE_BLOCKS * LANES - GENES), constant_values=-1)[None]
    far, far_at = gathered(rest, "y", "x")

    low = windows(order, places(near_at, "x", "y"), module, z, near)
    high = windows(order, places(far_at, "y", "x"), module, z, far)

    parts = jnp.concatenate([low.reshape(16, 16, MODULES), high.reshape(16, 24, MODULES)], axis=1)
    arrived = lax.all_to_all(parts, ("x", "y"), 0, 0, tiled=True).sum(axis=0)
    mine, others = arrived[:ROWS], arrived[ROWS : 2 * ROWS]
    straight, crossed = [], []
    for c in range(COHORTS):
        for g in range(32):
            straight.append((c * 32 + g, g * 8 + c))
    for c in range(COHORTS):
        for g in range(32):
            crossed.append((c * 32 + g, (g ^ 1) * 8 + c))
    first = lax.ppermute(mine, ALL_AXES, straight)
    second = lax.ppermute(others, ALL_AXES, crossed)
    return jnp.log1p(first + second)


def solution(mesh):
    finer = Mesh(mesh.devices.reshape(4, 2, 4, 4, 2), ALL_AXES)
    placed = (P(GENE_AXES, None), P(COHORT_AXES, None), P(GENE_AXES))
    return jax.shard_map(
        on_device, mesh=finer, in_specs=placed, out_specs=P(ALL_AXES, None), check_vma=False
    )
```

```python
import functools

import jax
import jax.numpy as jnp
from jax import lax
from jax.experimental import pallas as pl
from jax.experimental.pallas import tpu as pltpu
from jax.sharding import Mesh
from jax.sharding import PartitionSpec as P


MODULES = 128
COHORTS = 8
SAMPLES = 400
POOL = COHORTS * SAMPLES
GENES = 750
ROWS = 19
LANES = 128
TILES = POOL // LANES
DEPTH = 512
PITCH = POOL + 4
SHORT = SAMPLES + 4
CHUNK = 640
GENE_BLOCKS = 6
HALF = 3
COHORT_AXES = ("z_lo", "core")
GENE_AXES = ("x", "y", "z_hi")
ALL_AXES = COHORT_AXES + GENE_AXES
F32 = jnp.float32
BF16 = jnp.bfloat16


def transpose_in(load, blocks, turned, start, count):
    for k in range(start, start + count):
        for b in range(blocks):
            turned[b * PITCH + k * LANES : b * PITCH + (k + 1) * LANES, :] = load(b, k * LANES).T


def gather_cohort(order, cohort, turned, grouped, blocks):
    for u in range(SAMPLES):
        sample = order[cohort, u]
        grouped[pl.ds(u, blocks, stride=SHORT), :] = turned[pl.ds(sample, blocks, stride=PITCH), :]


def in_turn(order, turned, groups, blocks, finish):
    gather_cohort(order, 0, turned, groups[0], blocks)
    for c in range(COHORTS):
        if c + 1 < COHORTS:
            gather_cohort(order, c + 1, turned, groups[(c + 1) % 2], blocks)
        finish(c, c % 2)


def standardized(grouped, block):
    x = grouped[block * SHORT : block * SHORT + SAMPLES, :]
    centred = x - jnp.sum(x, axis=0, keepdims=True) * (1.0 / SAMPLES)
    spread = jnp.sqrt(jnp.sum(centred * centred, axis=0, keepdims=True) + 0.01 * SAMPLES)
    return centred * (1.0 / spread)


def gene_kernel(first, order, x_ref, z_ref, turned, even, odd):
    here = min(HALF * LANES, GENES - first * LANES)
    step = pl.program_id(0)

    for k in range(CHUNK // LANES):
        lane = pl.multiple_of(step * CHUNK, LANES) + k * LANES
        for b in range(HALF):
            rows = min(LANES, here - b * LANES)
            tile = x_ref[b * LANES : b * LANES + rows, k * LANES : (k + 1) * LANES].astype(F32)
            if rows < LANES:
                tile = jnp.concatenate([tile, jnp.zeros((LANES - rows, LANES), F32)], axis=0)
            turned[pl.ds(b * PITCH + lane, LANES), :] = tile.T

    def finish(c, slot):
        for b in range(HALF):
            z = standardized((even, odd)[slot], b)
            z = jnp.concatenate([z, jnp.zeros((DEPTH - SAMPLES, LANES), F32)], axis=0).astype(BF16)
            z_ref[c, b * LANES : (b + 1) * LANES, :] = z.T

    @pl.when(step == POOL // CHUNK - 1)
    def _():
        in_turn(order, turned, (even, odd), HALF, finish)


def genes(first, order, x):
    return pl.pallas_call(
        functools.partial(gene_kernel, first),
        grid=(POOL // CHUNK,),
        out_shape=jax.ShapeDtypeStruct((COHORTS, HALF * LANES, DEPTH), BF16),
        in_specs=[
            pl.BlockSpec(memory_space=pltpu.SMEM),
            pl.BlockSpec((HALF * LANES, CHUNK), lambda i: (first // HALF, i)),
        ],
        out_specs=pl.BlockSpec(memory_space=pltpu.VMEM),
        scratch_shapes=[
            pltpu.VMEM((HALF * PITCH, LANES), F32),
            pltpu.VMEM((HALF * SHORT, LANES), F32),
            pltpu.VMEM((HALF * SHORT, LANES), F32),
        ],
        compiler_params=pltpu.CompilerParams(vmem_limit_bytes=14 * 2**20),
    )(order, x)


def window_kernel(units, rows, order, place, module_ref, z_top, z_bottom, *refs):
    parts = refs[:units]
    out_ref, turned, even, odd, zw0, zw1, low, consensus = refs[units:]
    total = sum(p.shape[0] for p in parts) * rows
    blocks = total // LANES
    strips = [(p, j, r) for p in parts for j in range(p.shape[0]) for r in range(0, rows, 8)]

    def load(b, lane):
        return jnp.concatenate(
            [p[j, r : r + 8, lane : lane + LANES].astype(F32) for p, j, r in strips[b * 16 : (b + 1) * 16]],
            axis=0,
        )

    transpose_in(load, blocks, turned, 0, TILES)
    for zw in (zw0, zw1):
        zw[SAMPLES:, :] = jnp.zeros((DEPTH - SAMPLES, total), BF16)

    def finish(c, slot):
        zw = (zw0, zw1)[slot]
        for b in range(blocks):
            zw[:SAMPLES, b * LANES : (b + 1) * LANES] = standardized((even, odd)[slot], b).astype(BF16)
        for i, z_ref in enumerate((z_top, z_bottom)):
            half = slice(i * HALF * LANES, (i + 1) * HALF * LANES)
            corr = jnp.dot(z_ref[c], zw[...], preferred_element_type=F32)
            low[half, :] = jnp.minimum(low[half, :], corr) if c else corr

    in_turn(order, turned, (even, odd), blocks, finish)

    base = (1.0 + jnp.maximum(low[...], -1.0)) * 0.5
    square = base * base
    fourth = square * square
    consensus[...] = (fourth * fourth * fourth).astype(BF16)
    module = lax.broadcasted_iota(jnp.int32, (MODULES, GENE_BLOCKS * LANES), 0)
    onehot = jnp.where(module_ref[...] == module, 1.0, 0.0).astype(BF16)
    degree = jnp.dot(onehot, consensus[...], preferred_element_type=F32)
    turned_degree = degree.T
    for i in range(total // rows):
        at = pl.multiple_of(place[i] * rows, 8)
        out_ref[pl.ds(at, rows), :] = turned_degree[i * rows : (i + 1) * rows, :]


def windows(order, place, module, z, parts):
    rows = parts[0].shape[1]
    total = sum(p.shape[0] for p in parts) * rows
    blocks = total // LANES
    return pl.pallas_call(
        functools.partial(window_kernel, len(parts), rows),
        out_shape=jax.ShapeDtypeStruct((total, MODULES), F32),
        in_specs=[pl.BlockSpec(memory_space=pltpu.SMEM)] * 2
        + [pl.BlockSpec(memory_space=pltpu.VMEM)] * (3 + len(parts)),
        out_specs=pl.BlockSpec(memory_space=pltpu.VMEM),
        scratch_shapes=[
            pltpu.VMEM((blocks * PITCH, LANES), F32),
            pltpu.VMEM((blocks * SHORT, LANES), F32),
            pltpu.VMEM((blocks * SHORT, LANES), F32),
            pltpu.VMEM((DEPTH, total), BF16),
            pltpu.VMEM((DEPTH, total), BF16),
            pltpu.VMEM((GENE_BLOCKS * LANES, total), F32),
            pltpu.VMEM((GENE_BLOCKS * LANES, total), BF16),
        ],
        compiler_params=pltpu.CompilerParams(vmem_limit_bytes=20 * 2**20),
    )(order, place, module, *z, *parts)


def shifted(array, axis, by):
    n = lax.axis_size(axis)
    return lax.ppermute(array, axis, [(i, (i + by) % n) for i in range(n)])


def gathered(unit, first, second):
    line = [unit] + [shifted(unit, first, by) for by in (1, 3, 2)]
    stack = jnp.stack(line)
    ahead, behind = shifted(stack, second, 1), shifted(stack, second, 3)
    far = [shifted(ahead[:2], second, 1), shifted(behind[2:], second, 3)]
    parts = [stack, ahead, behind, *far]
    one = (0, -1, 1, 2)
    return parts, [(a, b) for b, many in ((0, one), (-1, one), (1, one), (2, one)) for a in many]


def places(where, first, second):
    spots = []
    for a, b in where:
        at = {first: (lax.axis_index(first) + a) % 4, second: (lax.axis_index(second) + b) % 4}
        spots.append(at["x"] * 4 + at["y"])
    return jnp.stack(spots).astype(jnp.int32)


def in_plane(expression, sample_index, gene_block):
    z_lo, core = lax.axis_index("z_lo"), lax.axis_index("core")
    share = z_lo * 2 + core
    mirror = (3 - z_lo) * 2 + core
    both = jnp.concatenate([sample_index, lax.ppermute(sample_index, "core", [(0, 1), (1, 0)])])
    theirs = lax.dynamic_slice(expression, (mirror * ROWS, 0), (ROWS, POOL))
    own = lax.dynamic_slice(expression, (share * ROWS, 0), (ROWS, POOL))
    pairs = [(z * 2 + h, (3 - z) * 2 + 1 - h) for z in range(4) for h in range(2)]
    across = lax.ppermute(theirs, ("z_lo", "z_hi"), pairs)
    order = jnp.concatenate([both] + [shifted(both, "z_lo", by) for by in (1, 2, 3)])

    near, near_at = gathered(own[:16], "x", "y")
    rest = jnp.concatenate([own[16:], across, jnp.zeros((2, POOL), BF16)])
    far, far_at = gathered(rest, "y", "x")
    z = [genes(0, order, expression), genes(HALF, order, expression)]
    module = jnp.pad(gene_block, (0, GENE_BLOCKS * LANES - GENES), constant_values=-1)[None]

    low = windows(order, places(near_at, "x", "y"), module, z, near)
    high = windows(order, places(far_at, "y", "x"), module, z, far)

    parts = jnp.concatenate([low.reshape(16, 16, MODULES), high.reshape(16, 24, MODULES)], axis=1)
    arrived = lax.all_to_all(parts, ("x", "y"), 0, 0, tiled=True).sum(axis=0)
    mine, others = arrived[:ROWS], arrived[ROWS : 2 * ROWS]
    straight, crossed = [], []
    for c in range(COHORTS):
        for g in range(32):
            straight.append((c * 32 + g, g * 8 + c))
    for c in range(COHORTS):
        for g in range(32):
            crossed.append((c * 32 + g, (g ^ 1) * 8 + c))
    first = lax.ppermute(mine, ALL_AXES, straight)
    second = lax.ppermute(others, ALL_AXES, crossed)
    return jnp.log1p(first + second)


def solution(mesh):
    finer = Mesh(mesh.devices.reshape(4, 2, 4, 4, 2), ALL_AXES)
    placed = (P(GENE_AXES, None), P(COHORT_AXES, None), P(GENE_AXES))
    return jax.shard_map(
        in_plane, mesh=finer, in_specs=placed, out_specs=P(ALL_AXES, None), check_vma=False
    )
```

```python
import functools

import jax
import jax.numpy as jnp
from jax import lax
from jax.experimental import pallas as pl
from jax.experimental.pallas import tpu as pltpu
from jax.sharding import Mesh
from jax.sharding import PartitionSpec as P


MODULES = 128
ROW_DEV = 152
COHORTS = 8
SAMPLES = 400
POOL = COHORTS * SAMPLES
GENES = 750
ROWS = 19
LANES = 128
TILES = POOL // LANES
DEPTH = 512
PITCH = POOL + 4
SHORT = SAMPLES + 4
CHUNK = 640
GENE_BLOCKS = 6
COHORT_AXES = ("z_lo", "core")
GENE_AXES = ("x", "y", "z_hi")
ALL_AXES = COHORT_AXES + GENE_AXES
F32 = jnp.float32
BF16 = jnp.bfloat16


def transpose_in(load, blocks, turned, start, count):
    for k in range(start, start + count):
        for b in range(blocks):
            turned[b * PITCH + k * LANES : b * PITCH + (k + 1) * LANES, :] = load(b, k * LANES).T


def gather_cohort(source, turned, grouped, blocks):
    for u in range(SAMPLES):
        sample = source[0][source[1], u]
        grouped[pl.ds(u, blocks, stride=SHORT), :] = turned[pl.ds(sample, blocks, stride=PITCH), :]


def in_turn(order, turned, groups, blocks, finish):
    gather_cohort(order[0], turned, groups[0], blocks)
    for c in range(COHORTS):
        if c + 1 < COHORTS:
            gather_cohort(order[c + 1], turned, groups[(c + 1) % 2], blocks)
        finish(c, c % 2)


def standardized(grouped, block):
    x = grouped[block * SHORT : block * SHORT + SAMPLES, :]
    centred = x - jnp.sum(x, axis=0, keepdims=True) * (1.0 / SAMPLES)
    spread = jnp.sqrt(jnp.sum(centred * centred, axis=0, keepdims=True) + 0.01 * SAMPLES)
    return centred * (1.0 / spread)


def order_of(refs):
    return [(ref, row) for ref in refs for row in range(2)]


def gene_kernel(*refs):
    lists, (x_hbm, z_ref, x_ref, turned, even, odd, arrive) = refs[:4], refs[4:]

    def fetch(i):
        lanes = pl.ds(pl.multiple_of(i * CHUNK, LANES), CHUNK)
        return pltpu.make_async_copy(x_hbm.at[:, lanes], x_ref.at[:, lanes], arrive.at[i])

    for i in range(POOL // CHUNK):
        fetch(i).start()

    def chunk(i, _):
        fetch(i).wait()
        for k in range(CHUNK // LANES):
            lane = pl.multiple_of(i * CHUNK, LANES) + k * LANES
            for b in range(GENE_BLOCKS):
                rows = min(LANES, GENES - b * LANES)
                tile = x_ref[b * LANES : b * LANES + rows, pl.ds(lane, LANES)].astype(F32)
                if rows < LANES:
                    tile = jnp.concatenate([tile, jnp.zeros((LANES - rows, LANES), F32)], axis=0)
                turned[pl.ds(b * PITCH + lane, LANES), :] = tile.T
        return _

    lax.fori_loop(0, POOL // CHUNK, chunk, 0)

    def finish(c, slot):
        for b in range(GENE_BLOCKS):
            z = standardized((even, odd)[slot], b)
            z = jnp.concatenate([z, jnp.zeros((DEPTH - SAMPLES, LANES), F32)], axis=0).astype(BF16)
            z_ref[c, b * LANES : (b + 1) * LANES, :] = z.T

    in_turn(order_of(lists), turned, (even, odd), GENE_BLOCKS, finish)


def genes(lists, x):
    return pl.pallas_call(
        gene_kernel,
        out_shape=jax.ShapeDtypeStruct((COHORTS, GENE_BLOCKS * LANES, DEPTH), BF16),
        in_specs=[pl.BlockSpec(memory_space=pltpu.SMEM)] * 4 + [pl.BlockSpec(memory_space=pltpu.HBM)],
        out_specs=pl.BlockSpec(memory_space=pltpu.VMEM),
        scratch_shapes=[
            pltpu.VMEM((GENES, POOL), BF16),
            pltpu.VMEM((GENE_BLOCKS * PITCH, LANES), F32),
            pltpu.VMEM((GENE_BLOCKS * SHORT, LANES), F32),
            pltpu.VMEM((GENE_BLOCKS * SHORT, LANES), F32),
            pltpu.SemaphoreType.DMA((POOL // CHUNK,)),
        ],
        compiler_params=pltpu.CompilerParams(vmem_limit_bytes=26 * 2**20),
        name="genes",
    )(*lists, x)


def pick_kernel(x_ref, near_ref, mine_ref, theirs_ref):
    z_lo, core = lax.axis_index("z_lo"), lax.axis_index("core")
    own = (z_lo * 2 + core) * ROWS
    other = ((3 - z_lo) * 2 + core) * ROWS
    row = lax.broadcasted_iota(jnp.int32, (64, ROW_DEV), 0)
    column = lax.broadcasted_iota(jnp.int32, (64, ROW_DEV), 1)
    wanted = jnp.where(
        row < 19, own + row, jnp.where((row >= 43) & (row < 62), other + row - 43, -1)
    )
    select = jnp.where(column == wanted, 1.0, 0.0).astype(BF16)
    rows = jnp.dot(select, x_ref[...], preferred_element_type=F32).astype(BF16)
    near_ref[...] = rows[:16]
    mine_ref[...] = rows[16:40]
    theirs_ref[...] = rows[40:]


def pick(x):
    return pl.pallas_call(
        pick_kernel,
        out_shape=[jax.ShapeDtypeStruct((rows, POOL), BF16) for rows in (16, 24, 24)],
        in_specs=[pl.BlockSpec(memory_space=pltpu.VMEM)],
        out_specs=[pl.BlockSpec(memory_space=pltpu.VMEM)] * 3,
        compiler_params=pltpu.CompilerParams(vmem_limit_bytes=6 * 2**20),
        name="pick",
    )(x)


def window_kernel(units, rows, axes, where, before, *refs):
    lists, (module_ref, z_ref), refs = refs[:4], refs[4:6], refs[6:]
    early, parts, refs = refs[:before], refs[before : before + units], refs[before + units :]
    out_ref, turned, even, odd, zw0, zw1, low, consensus, label = refs
    total = sum(p.shape[0] for p in parts) * rows
    blocks = total // LANES
    strips = [(p, j, r) for p in parts for j in range(p.shape[0]) for r in range(0, rows, 8)]

    def load(b, lane):
        return jnp.concatenate(
            [p[j, r : r + 8, lane : lane + LANES].astype(F32) for p, j, r in strips[b * 16 : (b + 1) * 16]],
            axis=0,
        )

    transpose_in(load, blocks, turned, 0, TILES)
    for zw in (zw0, zw1):
        zw[SAMPLES:, :] = jnp.zeros((DEPTH - SAMPLES, total), BF16)

    def finish(c, slot):
        zw = (zw0, zw1)[slot]
        for b in range(blocks):
            zw[:SAMPLES, b * LANES : (b + 1) * LANES] = standardized((even, odd)[slot], b).astype(BF16)
        corr = jnp.dot(z_ref[c], zw[...], preferred_element_type=F32)
        low[...] = jnp.minimum(low[...], corr) if c else corr

    in_turn(order_of(lists), turned, (even, odd), blocks, finish)

    base = (1.0 + jnp.maximum(low[...], -1.0)) * 0.5
    square = base * base
    fourth = square * square
    consensus[...] = (fourth * fourth * fourth).astype(BF16)
    label[...] = jnp.full(label.shape, -1, jnp.int32)
    label[:, :GENES] = module_ref[...]
    module = lax.broadcasted_iota(jnp.int32, (MODULES, GENE_BLOCKS * LANES), 0)
    onehot = jnp.where(label[...] == module, 1.0, 0.0).astype(BF16)
    degree = jnp.dot(onehot, consensus[...], preferred_element_type=F32).T
    first, second = (lax.axis_index(axis) for axis in axes)
    for i, (a, b) in enumerate(where):
        spot = {axes[0]: lax.rem(first + a + 4, 4), axes[1]: lax.rem(second + b + 4, 4)}
        out_ref[spot["x"] * 4 + spot["y"], before * 16 : before * 16 + rows, :] = degree[
            i * rows : (i + 1) * rows, :
        ]
    if before:
        out_ref[:, :16, :] = early[0][...]


def windows(lists, module, z, parts, axes, where, early=()):
    rows = parts[0].shape[1]
    total = sum(p.shape[0] for p in parts) * rows
    blocks = total // LANES
    return pl.pallas_call(
        functools.partial(window_kernel, len(parts), rows, axes, where, len(early)),
        out_shape=jax.ShapeDtypeStruct((16, rows + 16 * len(early), MODULES), F32),
        in_specs=[pl.BlockSpec(memory_space=pltpu.SMEM)] * 4
        + [pl.BlockSpec(memory_space=pltpu.VMEM)] * (2 + len(early) + len(parts)),
        out_specs=pl.BlockSpec(memory_space=pltpu.VMEM),
        scratch_shapes=[
            pltpu.VMEM((blocks * PITCH, LANES), F32),
            pltpu.VMEM((blocks * SHORT, LANES), F32),
            pltpu.VMEM((blocks * SHORT, LANES), F32),
            pltpu.VMEM((DEPTH, total), BF16),
            pltpu.VMEM((DEPTH, total), BF16),
            pltpu.VMEM((GENE_BLOCKS * LANES, total), F32),
            pltpu.VMEM((GENE_BLOCKS * LANES, total), BF16),
            pltpu.VMEM((1, GENE_BLOCKS * LANES), jnp.int32),
        ],
        compiler_params=pltpu.CompilerParams(vmem_limit_bytes=20 * 2**20),
    )(*lists, module, z, *early, *parts)


def shifted(array, axis, by):
    n = lax.axis_size(axis)
    return lax.ppermute(array, axis, [(i, (i + by) % n) for i in range(n)])


def gathered(unit, first, second):
    line = [unit] + [shifted(unit, first, by) for by in (1, 3, 2)]
    stack = jnp.stack(line)
    ahead, behind = shifted(stack, second, 1), shifted(stack, second, 3)
    far = [shifted(ahead[:2], second, 1), shifted(behind[2:], second, 3)]
    parts = [stack, ahead, behind, *far]
    one = (0, -1, 1, 2)
    return parts, [(a, b) for b, many in ((0, one), (-1, one), (1, one), (2, one)) for a in many]


def in_plane(expression, sample_index, gene_block):
    own, mine, theirs = pick(expression[:ROW_DEV])
    both = jnp.concatenate([sample_index, lax.ppermute(sample_index, "core", [(0, 1), (1, 0)])])
    pairs = [(z * 2 + h, (3 - z) * 2 + 1 - h) for z in range(4) for h in range(2)]
    across = lax.ppermute(theirs, ("z_lo", "z_hi"), pairs)
    lists = [both] + [shifted(both, "z_lo", by) for by in (1, 2, 3)]

    near, near_at = gathered(own, "x", "y")
    far, far_at = gathered(mine + across, "y", "x")
    z = genes(lists, expression)
    module = gene_block.reshape(1, GENES)

    low = windows(lists, module, z, near, ("x", "y"), near_at)
    parts = windows(lists, module, z, far, ("y", "x"), far_at, (low,))

    arrived = lax.all_to_all(parts, ("x", "y"), 0, 0, tiled=True).sum(axis=0)
    mine, others = arrived[:ROWS], arrived[ROWS : 2 * ROWS]
    straight, crossed = [], []
    for c in range(COHORTS):
        for g in range(32):
            straight.append((c * 32 + g, g * 8 + c))
    for c in range(COHORTS):
        for g in range(32):
            crossed.append((c * 32 + g, (g ^ 1) * 8 + c))
    first = lax.ppermute(mine, ALL_AXES, straight)
    second = lax.ppermute(others, ALL_AXES, crossed)
    return jnp.log1p(first + second)


def solution(mesh):
    finer = Mesh(mesh.devices.reshape(4, 2, 4, 4, 2), ALL_AXES)
    placed = (P(GENE_AXES, None), P(COHORT_AXES, None), P(GENE_AXES))
    return jax.shard_map(in_plane, mesh=finer, in_specs=placed, out_specs=P(ALL_AXES, None), check_vma=False)
```

```python
import functools

import jax
import jax.numpy as jnp
from jax import lax
from jax.experimental import pallas as pl
from jax.experimental.pallas import tpu as pltpu
from jax.sharding import Mesh
from jax.sharding import PartitionSpec as P


MODULES = 128
ROW_DEV = 152
COHORTS = 8
SAMPLES = 400
POOL = COHORTS * SAMPLES
GENES = 750
ROWS = 19
SLOT = 24
LANES = 128
DEPTH = 512
PITCH = POOL + 4
SHORT = SAMPLES + 4
CHUNK = 640
GENE_BLOCKS = 6
COHORT_AXES = ("z_lo", "core")
GENE_AXES = ("x", "y", "z_hi")
ALL_AXES = COHORT_AXES + GENE_AXES
F32 = jnp.float32
BF16 = jnp.bfloat16


def transpose_in(load, blocks, turned):
    def chunk(i, _):
        for k in range(CHUNK // LANES):
            lane = pl.multiple_of(i * CHUNK, LANES) + k * LANES
            for b in range(blocks):
                turned[pl.ds(b * PITCH + lane, LANES), :] = load(b, lane).T
        return _

    lax.fori_loop(0, POOL // CHUNK, chunk, 0)


def gather_cohort(source, turned, grouped, blocks):
    for u in range(SAMPLES):
        sample = source[0][source[1], u]
        grouped[pl.ds(u, blocks, stride=SHORT), :] = turned[pl.ds(sample, blocks, stride=PITCH), :]


def in_turn(order, turned, groups, blocks, finish):
    gather_cohort(order[0], turned, groups[0], blocks)
    for c in range(COHORTS):
        if c + 1 < COHORTS:
            gather_cohort(order[c + 1], turned, groups[(c + 1) % 2], blocks)
        finish(c, c % 2)


def standardized(grouped, block):
    x = grouped[block * SHORT : block * SHORT + SAMPLES, :]
    centred = x - jnp.sum(x, axis=0, keepdims=True) * (1.0 / SAMPLES)
    spread = jnp.sqrt(jnp.sum(centred * centred, axis=0, keepdims=True) + 0.01 * SAMPLES)
    return centred * (1.0 / spread)


def order_of(refs):
    return [(ref, row) for ref in refs for row in range(2)]


def gene_kernel(*refs):
    lists, (x_hbm, z_ref, x_ref, turned, even, odd, arrive) = refs[:4], refs[4:]

    def fetch(i):
        lanes = pl.ds(pl.multiple_of(i * CHUNK, LANES), CHUNK)
        return pltpu.make_async_copy(x_hbm.at[:, lanes], x_ref.at[:, lanes], arrive.at[i])

    for i in range(POOL // CHUNK):
        fetch(i).start()

    def chunk(i, _):
        fetch(i).wait()
        for k in range(CHUNK // LANES):
            lane = pl.multiple_of(i * CHUNK, LANES) + k * LANES
            for b in range(GENE_BLOCKS):
                rows = min(LANES, GENES - b * LANES)
                tile = x_ref[b * LANES : b * LANES + rows, pl.ds(lane, LANES)].astype(F32)
                if rows < LANES:
                    tile = jnp.concatenate([tile, jnp.zeros((LANES - rows, LANES), F32)], axis=0)
                turned[pl.ds(b * PITCH + lane, LANES), :] = tile.T
        return _

    lax.fori_loop(0, POOL // CHUNK, chunk, 0)

    def finish(c, slot):
        for b in range(GENE_BLOCKS):
            z = standardized((even, odd)[slot], b)
            z = jnp.concatenate([z, jnp.zeros((DEPTH - SAMPLES, LANES), F32)], axis=0).astype(BF16)
            z_ref[c, b * LANES : (b + 1) * LANES, :] = z.T

    in_turn(order_of(lists), turned, (even, odd), GENE_BLOCKS, finish)


def genes(lists, x):
    return pl.pallas_call(
        gene_kernel,
        out_shape=jax.ShapeDtypeStruct((COHORTS, GENE_BLOCKS * LANES, DEPTH), BF16),
        in_specs=[pl.BlockSpec(memory_space=pltpu.SMEM)] * 4 + [pl.BlockSpec(memory_space=pltpu.HBM)],
        out_specs=pl.BlockSpec(memory_space=pltpu.VMEM),
        scratch_shapes=[
            pltpu.VMEM((GENES, POOL), BF16),
            pltpu.VMEM((GENE_BLOCKS * PITCH, LANES), F32),
            pltpu.VMEM((GENE_BLOCKS * SHORT, LANES), F32),
            pltpu.VMEM((GENE_BLOCKS * SHORT, LANES), F32),
            pltpu.SemaphoreType.DMA((POOL // CHUNK,)),
        ],
        compiler_params=pltpu.CompilerParams(vmem_limit_bytes=26 * 2**20),
        name="genes",
    )(*lists, x)


def share_of(cohort, x, y):
    return lax.rem(cohort + x * 2 + y // 2, COHORTS)


def pick_kernel(x_hbm, near_ref, mine_ref, theirs_ref, x_ref, arrive):
    copy = pltpu.make_async_copy(x_hbm.at[pl.ds(0, ROW_DEV), :], x_ref, arrive)
    copy.start()
    z_lo, core = lax.axis_index("z_lo"), lax.axis_index("core")
    x, y = lax.axis_index("x"), lax.axis_index("y")
    own = share_of(z_lo * 2 + core, x, y) * ROWS
    other = share_of((3 - z_lo) * 2 + core, x, y) * ROWS
    row = lax.broadcasted_iota(jnp.int32, (64, ROW_DEV), 0)
    column = lax.broadcasted_iota(jnp.int32, (64, ROW_DEV), 1)
    wanted = jnp.where(
        row < 19, own + row, jnp.where((row >= 43) & (row < 62), other + row - 43, -1)
    )
    select = jnp.where(column == wanted, 1.0, 0.0).astype(BF16)
    copy.wait()
    rows = jnp.dot(select, x_ref[...], preferred_element_type=F32).astype(BF16)
    near_ref[...] = rows[:16]
    mine_ref[...] = rows[16:40]
    theirs_ref[...] = rows[40:]


def pick(x):
    return pl.pallas_call(
        pick_kernel,
        out_shape=[jax.ShapeDtypeStruct((rows, POOL), BF16) for rows in (16, 24, 24)],
        in_specs=[pl.BlockSpec(memory_space=pltpu.HBM)],
        out_specs=[pl.BlockSpec(memory_space=pltpu.VMEM)] * 3,
        scratch_shapes=[pltpu.VMEM((ROW_DEV, POOL), BF16), pltpu.SemaphoreType.DMA(())],
        compiler_params=pltpu.CompilerParams(vmem_limit_bytes=6 * 2**20),
        name="pick",
    )(x)


def window_kernel(units, spots, done, *refs):
    lists, (module_ref, z_ref), refs = refs[:4], refs[4:6], refs[6:]
    before, parts, refs = refs[: len(done)], refs[len(done) : len(done) + units], refs[len(done) + units :]
    out_ref, turned, even, odd, zw0, zw1, low, consensus, label, raw = refs
    total = low.shape[1]
    blocks = total // LANES
    strips = [(p, j, r) for p in parts for j in range(p.shape[0]) for r in range(0, p.shape[1], 8)]

    def load(b, lane):
        mine = strips[b * 16 : (b + 1) * 16]
        tiles = [p[j, r : r + 8, pl.ds(lane, LANES)].astype(F32) for p, j, r in mine]
        return jnp.concatenate(tiles + [jnp.zeros((8, LANES), F32)] * (16 - len(mine)), axis=0)

    transpose_in(load, blocks, turned)
    for zw in (zw0, zw1):
        zw[SAMPLES:, :] = jnp.zeros((DEPTH - SAMPLES, total), BF16)

    def finish(c, slot):
        zw = (zw0, zw1)[slot]
        for b in range(blocks):
            zw[:SAMPLES, b * LANES : (b + 1) * LANES] = standardized((even, odd)[slot], b).astype(BF16)
        corr = jnp.dot(z_ref[c], zw[...], preferred_element_type=F32)
        low[...] = jnp.minimum(low[...], corr) if c else corr

    in_turn(order_of(lists), turned, (even, odd), blocks, finish)

    base = (1.0 + jnp.maximum(low[...], -1.0)) * 0.5
    square = base * base
    fourth = square * square
    consensus[...] = (fourth * fourth * fourth).astype(BF16)
    label[...] = jnp.full(label.shape, -1, jnp.int32)
    label[:, :GENES] = module_ref[...]
    module = lax.broadcasted_iota(jnp.int32, (MODULES, GENE_BLOCKS * LANES), 0)
    onehot = jnp.where(label[...] == module, 1.0, 0.0).astype(BF16)
    degree = jnp.dot(onehot, consensus[...], preferred_element_type=F32).T
    if not done:
        out_ref[...] = degree
        return
    raw[...] = degree
    deal([*before, raw], [*done, spots], out_ref)


def deal(sums, spots, out_ref):
    x, y, z_hi = (lax.axis_index(axis) for axis in GENE_AXES)
    cohort = lax.axis_index("z_lo") * 2 + lax.axis_index("core")
    for ref, units in zip(sums, spots, strict=True):
        for row, rows, dx, dy in units:
            from_x, from_y = lax.rem(x + dx + 4, 4), lax.rem(y + dy + 4, 4)
            share = share_of(cohort, from_x, from_y)
            half = (from_y % 2) * 2
            own = (half + z_hi) * 4 + share // 2
            other = (half + 1 - z_hi) * 4 + share // 2
            at = pl.multiple_of((share % 2) * SLOT, 8)
            if rows == 16:
                out_ref[own, pl.ds(at, 16), :] = ref[row : row + 16, :]
            else:
                out_ref[own, pl.ds(at + 16, 3), :] = ref[row : row + 3, :]
                out_ref[other, pl.ds(at, ROWS), :] = ref[row + 3 : row + 3 + ROWS, :]


def windows(lists, module, z, parts, spots, done=(), sums=()):
    total = -(-sum(p.shape[0] * p.shape[1] for p in parts) // LANES) * LANES
    blocks = total // LANES
    shape = (16, 2 * SLOT, MODULES) if done else (total, MODULES)
    return pl.pallas_call(
        functools.partial(window_kernel, len(parts), spots, done),
        out_shape=jax.ShapeDtypeStruct(shape, F32),
        in_specs=[pl.BlockSpec(memory_space=pltpu.SMEM)] * 4
        + [pl.BlockSpec(memory_space=pltpu.VMEM)] * (2 + len(sums) + len(parts)),
        out_specs=pl.BlockSpec(memory_space=pltpu.VMEM),
        scratch_shapes=[
            pltpu.VMEM((blocks * PITCH, LANES), F32),
            pltpu.VMEM((blocks * SHORT, LANES), F32),
            pltpu.VMEM((blocks * SHORT, LANES), F32),
            pltpu.VMEM((DEPTH, total), BF16),
            pltpu.VMEM((DEPTH, total), BF16),
            pltpu.VMEM((GENE_BLOCKS * LANES, total), F32),
            pltpu.VMEM((GENE_BLOCKS * LANES, total), BF16),
            pltpu.VMEM((1, GENE_BLOCKS * LANES), jnp.int32),
            pltpu.VMEM((total, MODULES), F32),
        ],
        compiler_params=pltpu.CompilerParams(vmem_limit_bytes=20 * 2**20),
    )(*lists, module, z, *sums, *parts)


def shifted(array, axis, by):
    n = lax.axis_size(axis)
    return lax.ppermute(array, axis, [(i, (i + by) % n) for i in range(n)])


def gathered(unit, first, second):
    line = [unit] + [shifted(unit, first, by) for by in (1, 3, 2)]
    stack = jnp.stack(line)
    ahead, behind = shifted(stack, second, 1), shifted(stack, second, 3)
    far = [shifted(ahead[:2], second, 1), shifted(behind[2:], second, 3)]
    one = (0, -1, 1, 2)
    where = [[(a, 0) for a in one], [(a, -1) for a in one], [(a, 1) for a in one]]
    where += [[(a, 2) for a in one[:2]], [(a, 2) for a in one[2:]]]
    if first == "y":
        where = [[(b, a) for a, b in many] for many in where]
    return list(zip([stack, ahead, behind, *far], where, strict=True))


def laid(parts):
    spots, row = [], 0
    for array, where in parts:
        for dx, dy in where:
            spots.append((row, array.shape[1], dx, dy))
            row += array.shape[1]
    return [array for array, _ in parts], tuple(spots)


def in_plane(expression, sample_index, gene_block):
    own, mine, theirs = pick(expression)
    both = jnp.concatenate([sample_index, lax.ppermute(sample_index, "core", [(0, 1), (1, 0)])])
    pairs = [(z * 2 + h, (3 - z) * 2 + 1 - h) for z in range(4) for h in range(2)]
    across = lax.ppermute(theirs, ("z_lo", "z_hi"), pairs)
    lists = [both] + [shifted(both, "z_lo", by) for by in (1, 2, 3)]

    near = gathered(own, "x", "y")
    far = gathered(mine + across, "y", "x")
    z = genes(lists, expression)
    module = gene_block.reshape(1, GENES)

    parts, spots_0 = laid(near[:3] + far[:1])
    sums_0 = windows(lists, module, z, parts, spots_0)
    parts, spots_1 = laid(near[3:] + far[1:3])
    sums_1 = windows(lists, module, z, parts, spots_1)
    parts, spots_2 = laid(far[3:])
    dealt = windows(lists, module, z, parts, spots_2, (spots_0, spots_1), (sums_0, sums_1))

    arrived = lax.all_to_all(dealt, ("x", "y"), 0, 0, tiled=True).sum(axis=0)
    arrived = arrived.reshape(2, SLOT, MODULES)[:, :ROWS]
    z_hi = lax.axis_index("z_hi")
    first = lax.ppermute(lax.dynamic_index_in_dim(arrived, z_hi, 0, False), ALL_AXES, home(0))
    second = lax.ppermute(lax.dynamic_index_in_dim(arrived, 1 - z_hi, 0, False), ALL_AXES, home(1))
    return jnp.log1p(first + second)


def home(flip):
    pairs = []
    for c in range(COHORTS):
        for x in range(4):
            for y in range(4):
                for z_hi in range(2):
                    slot = z_hi ^ flip
                    there = (2 * y + slot - c) % COHORTS
                    pairs.append((c * 32 + (x * 4 + y) * 2 + z_hi, there * 32 + (x * 4 + y) * 2 + slot))
    return pairs


def solution(mesh):
    finer = Mesh(mesh.devices.reshape(4, 2, 4, 4, 2), ALL_AXES)
    placed = (P(GENE_AXES, None), P(COHORT_AXES, None), P(GENE_AXES))
    return jax.shard_map(in_plane, mesh=finer, in_specs=placed, out_specs=P(ALL_AXES, None), check_vma=False)
```

```python
import functools

import jax
import jax.numpy as jnp
from jax import lax
from jax.experimental import pallas as pl
from jax.experimental.pallas import tpu as pltpu
from jax.sharding import Mesh
from jax.sharding import PartitionSpec as P


MODULES = 128
ROW_DEV = 152
COHORTS = 8
SAMPLES = 400
POOL = COHORTS * SAMPLES
GENES = 750
ROWS = 19
SLOT = 24
LANES = 128
DEPTH = 512
PITCH = POOL + 4
SHORT = SAMPLES + 4
CHUNK = 640
GENE_BLOCKS = 6
COHORT_AXES = ("z_lo", "core")
GENE_AXES = ("x", "y", "z_hi")
ALL_AXES = COHORT_AXES + GENE_AXES
F32 = jnp.float32
BF16 = jnp.bfloat16


def transpose_in(load, blocks, turned):
    def chunk(i, _):
        for k in range(CHUNK // LANES):
            lane = pl.multiple_of(i * CHUNK, LANES) + k * LANES
            for b in range(blocks):
                turned[pl.ds(b * PITCH + lane, LANES), :] = load(b, lane).T
        return _

    lax.fori_loop(0, POOL // CHUNK, chunk, 0)


def gather_cohort(source, turned, grouped, blocks):
    for u in range(SAMPLES):
        sample = source[0][source[1], u]
        grouped[pl.ds(u, blocks, stride=SHORT), :] = turned[pl.ds(sample, blocks, stride=PITCH), :]


def in_turn(order, turned, groups, blocks, finish):
    gather_cohort(order[0], turned, groups[0], blocks)
    for c in range(COHORTS):
        if c + 1 < COHORTS:
            gather_cohort(order[c + 1], turned, groups[(c + 1) % 2], blocks)
        finish(c, c % 2)


def standardized(grouped, block):
    x = grouped[block * SHORT : block * SHORT + SAMPLES, :]
    centred = x - jnp.sum(x, axis=0, keepdims=True) * (1.0 / SAMPLES)
    spread = jnp.sqrt(jnp.sum(centred * centred, axis=0, keepdims=True) + 0.01 * SAMPLES)
    return centred * (1.0 / spread)


def order_of(refs):
    return [(ref, row) for ref in refs for row in range(2)]


def brought(lists, here, ready):
    return [pltpu.make_async_copy(a, b, ready.at[i]) for i, (a, b) in enumerate(zip(lists, here, strict=True))]


def list_scratch():
    return [pltpu.SMEM((2, SAMPLES), jnp.int32)] * 4 + [pltpu.SemaphoreType.DMA((4,))]


def gene_kernel(*refs):
    lists, (x_hbm, z_ref, x_ref, turned, even, odd, arrive, *here, ready) = refs[:4], refs[4:]
    for copy in brought(lists, here, ready):
        copy.start()

    def fetch(i):
        lanes = pl.ds(pl.multiple_of(i * CHUNK, LANES), CHUNK)
        return pltpu.make_async_copy(x_hbm.at[:, lanes], x_ref.at[:, lanes], arrive.at[i])

    for i in range(POOL // CHUNK):
        fetch(i).start()

    def chunk(i, _):
        fetch(i).wait()
        for k in range(CHUNK // LANES):
            lane = pl.multiple_of(i * CHUNK, LANES) + k * LANES
            for b in range(GENE_BLOCKS):
                rows = min(LANES, GENES - b * LANES)
                tile = x_ref[b * LANES : b * LANES + rows, pl.ds(lane, LANES)].astype(F32)
                if rows < LANES:
                    tile = jnp.concatenate([tile, jnp.zeros((LANES - rows, LANES), F32)], axis=0)
                turned[pl.ds(b * PITCH + lane, LANES), :] = tile.T
        return _

    lax.fori_loop(0, POOL // CHUNK, chunk, 0)

    def finish(c, slot):
        for b in range(GENE_BLOCKS):
            z = standardized((even, odd)[slot], b)
            z = jnp.concatenate([z, jnp.zeros((DEPTH - SAMPLES, LANES), F32)], axis=0).astype(BF16)
            z_ref[c, b * LANES : (b + 1) * LANES, :] = z.T

    for copy in brought(lists, here, ready):
        copy.wait()
    in_turn(order_of(here), turned, (even, odd), GENE_BLOCKS, finish)


def genes(lists, x):
    return pl.pallas_call(
        gene_kernel,
        out_shape=jax.ShapeDtypeStruct((COHORTS, GENE_BLOCKS * LANES, DEPTH), BF16),
        in_specs=[pl.BlockSpec(memory_space=pl.ANY)] * 4 + [pl.BlockSpec(memory_space=pltpu.HBM)],
        out_specs=pl.BlockSpec(memory_space=pltpu.VMEM),
        scratch_shapes=[
            pltpu.VMEM((GENES, POOL), BF16),
            pltpu.VMEM((GENE_BLOCKS * PITCH, LANES), F32),
            pltpu.VMEM((GENE_BLOCKS * SHORT, LANES), F32),
            pltpu.VMEM((GENE_BLOCKS * SHORT, LANES), F32),
            pltpu.SemaphoreType.DMA((POOL // CHUNK,)),
            *list_scratch(),
        ],
        compiler_params=pltpu.CompilerParams(vmem_limit_bytes=26 * 2**20),
        name="genes",
    )(*lists, x)


def share_of(cohort, x, y):
    return lax.rem(cohort + x * 2 + y // 2, COHORTS)


def pick_kernel(x_hbm, near_ref, mine_ref, theirs_ref, x_ref, arrive):
    copy = pltpu.make_async_copy(x_hbm.at[pl.ds(0, ROW_DEV), :], x_ref, arrive)
    copy.start()
    z_lo, core = lax.axis_index("z_lo"), lax.axis_index("core")
    x, y = lax.axis_index("x"), lax.axis_index("y")
    own = share_of(z_lo * 2 + core, x, y) * ROWS
    other = share_of((3 - z_lo) * 2 + core, x, y) * ROWS
    row = lax.broadcasted_iota(jnp.int32, (64, ROW_DEV), 0)
    column = lax.broadcasted_iota(jnp.int32, (64, ROW_DEV), 1)
    wanted = jnp.where(
        row < 19, own + row, jnp.where((row >= 43) & (row < 62), other + row - 43, -1)
    )
    select = jnp.where(column == wanted, 1.0, 0.0).astype(BF16)
    copy.wait()
    rows = jnp.dot(select, x_ref[...], preferred_element_type=F32).astype(BF16)
    near_ref[...] = rows[:16]
    mine_ref[...] = rows[16:40]
    theirs_ref[...] = rows[40:]


def pick(x):
    return pl.pallas_call(
        pick_kernel,
        out_shape=[jax.ShapeDtypeStruct((rows, POOL), BF16) for rows in (16, 24, 24)],
        in_specs=[pl.BlockSpec(memory_space=pltpu.HBM)],
        out_specs=[pl.BlockSpec(memory_space=pltpu.VMEM)] * 3,
        scratch_shapes=[pltpu.VMEM((ROW_DEV, POOL), BF16), pltpu.SemaphoreType.DMA(())],
        compiler_params=pltpu.CompilerParams(vmem_limit_bytes=6 * 2**20),
        name="pick",
    )(x)


def window_kernel(units, spots, done, *refs):
    lists, (module_ref, z_ref), refs = refs[:4], refs[4:6], refs[6:]
    before, parts, refs = refs[: len(done)], refs[len(done) : len(done) + units], refs[len(done) + units :]
    out_ref, turned, even, odd, zw0, zw1, low, consensus, label, raw, *here, ready = refs
    for copy in brought(lists, here, ready):
        copy.start()
    total = low.shape[1]
    blocks = total // LANES
    strips = [(p, j, r) for p in parts for j in range(p.shape[0]) for r in range(0, p.shape[1], 8)]

    def load(b, lane):
        mine = strips[b * 16 : (b + 1) * 16]
        tiles = [p[j, r : r + 8, pl.ds(lane, LANES)].astype(F32) for p, j, r in mine]
        return jnp.concatenate(tiles + [jnp.zeros((8, LANES), F32)] * (16 - len(mine)), axis=0)

    transpose_in(load, blocks, turned)
    for zw in (zw0, zw1):
        zw[SAMPLES:, :] = jnp.zeros((DEPTH - SAMPLES, total), BF16)

    def finish(c, slot):
        zw = (zw0, zw1)[slot]
        for b in range(blocks):
            zw[:SAMPLES, b * LANES : (b + 1) * LANES] = standardized((even, odd)[slot], b).astype(BF16)
        corr = jnp.dot(z_ref[c], zw[...], preferred_element_type=F32)
        low[...] = jnp.minimum(low[...], corr) if c else corr

    for copy in brought(lists, here, ready):
        copy.wait()
    in_turn(order_of(here), turned, (even, odd), blocks, finish)

    base = (1.0 + jnp.maximum(low[...], -1.0)) * 0.5
    square = base * base
    fourth = square * square
    consensus[...] = (fourth * fourth * fourth).astype(BF16)
    label[...] = jnp.full(label.shape, -1, jnp.int32)
    label[:, :GENES] = module_ref[...]
    module = lax.broadcasted_iota(jnp.int32, (MODULES, GENE_BLOCKS * LANES), 0)
    onehot = jnp.where(label[...] == module, 1.0, 0.0).astype(BF16)
    degree = jnp.dot(onehot, consensus[...], preferred_element_type=F32).T
    if not done:
        out_ref[...] = degree
        return
    raw[...] = degree
    deal([*before, raw], [*done, spots], out_ref)


def deal(sums, spots, out_ref):
    x, y, z_hi = (lax.axis_index(axis) for axis in GENE_AXES)
    cohort = lax.axis_index("z_lo") * 2 + lax.axis_index("core")
    for ref, units in zip(sums, spots, strict=True):
        for row, rows, dx, dy in units:
            from_x, from_y = lax.rem(x + dx + 4, 4), lax.rem(y + dy + 4, 4)
            share = share_of(cohort, from_x, from_y)
            half = (from_y % 2) * 2
            own = (half + z_hi) * 4 + share // 2
            other = (half + 1 - z_hi) * 4 + share // 2
            at = pl.multiple_of((share % 2) * SLOT, 8)
            if rows == 16:
                out_ref[own, pl.ds(at, 16), :] = ref[row : row + 16, :]
            else:
                out_ref[own, pl.ds(at + 16, 3), :] = ref[row : row + 3, :]
                out_ref[other, pl.ds(at, ROWS), :] = ref[row + 3 : row + 3 + ROWS, :]


def windows(lists, module, z, parts, spots, done=(), sums=()):
    total = -(-sum(p.shape[0] * p.shape[1] for p in parts) // LANES) * LANES
    blocks = total // LANES
    shape = (16, 2 * SLOT, MODULES) if done else (total, MODULES)
    return pl.pallas_call(
        functools.partial(window_kernel, len(parts), spots, done),
        out_shape=jax.ShapeDtypeStruct(shape, F32),
        in_specs=[pl.BlockSpec(memory_space=pl.ANY)] * 4
        + [pl.BlockSpec(memory_space=pltpu.VMEM)] * (2 + len(sums) + len(parts)),
        out_specs=pl.BlockSpec(memory_space=pltpu.VMEM),
        scratch_shapes=[
            pltpu.VMEM((blocks * PITCH, LANES), F32),
            pltpu.VMEM((blocks * SHORT, LANES), F32),
            pltpu.VMEM((blocks * SHORT, LANES), F32),
            pltpu.VMEM((DEPTH, total), BF16),
            pltpu.VMEM((DEPTH, total), BF16),
            pltpu.VMEM((GENE_BLOCKS * LANES, total), F32),
            pltpu.VMEM((GENE_BLOCKS * LANES, total), BF16),
            pltpu.VMEM((1, GENE_BLOCKS * LANES), jnp.int32),
            pltpu.VMEM((total, MODULES), F32),
            *list_scratch(),
        ],
        compiler_params=pltpu.CompilerParams(vmem_limit_bytes=20 * 2**20),
    )(*lists, module, z, *sums, *parts)


def shifted(array, axis, by):
    n = lax.axis_size(axis)
    return lax.ppermute(array, axis, [(i, (i + by) % n) for i in range(n)])


def gathered(unit, first, second):
    line = [unit] + [shifted(unit, first, by) for by in (1, 3, 2)]
    stack = jnp.stack(line)
    ahead, behind = shifted(stack, second, 1), shifted(stack, second, 3)
    far = [shifted(ahead[:2], second, 1), shifted(behind[2:], second, 3)]
    one = (0, -1, 1, 2)
    where = [[(a, 0) for a in one], [(a, -1) for a in one], [(a, 1) for a in one]]
    where += [[(a, 2) for a in one[:2]], [(a, 2) for a in one[2:]]]
    if first == "y":
        where = [[(b, a) for a, b in many] for many in where]
    return list(zip([stack, ahead, behind, *far], where, strict=True))


def laid(parts):
    spots, row = [], 0
    for array, where in parts:
        for dx, dy in where:
            spots.append((row, array.shape[1], dx, dy))
            row += array.shape[1]
    return [array for array, _ in parts], tuple(spots)


def in_plane(expression, sample_index, gene_block):
    own, mine, theirs = pick(expression)
    both = jnp.concatenate([sample_index, lax.ppermute(sample_index, "core", [(0, 1), (1, 0)])])
    pairs = [(z * 2 + h, (3 - z) * 2 + 1 - h) for z in range(4) for h in range(2)]
    across = lax.ppermute(theirs, ("z_lo", "z_hi"), pairs)
    lists = [both] + [shifted(both, "z_lo", by) for by in (1, 2, 3)]

    near = gathered(own, "x", "y")
    mine, stack = lax.optimization_barrier((mine, near[0][0]))
    near[0] = (stack, near[0][1])
    far = gathered(mine + across, "y", "x")
    z = genes(lists, expression)
    module = gene_block.reshape(1, GENES)

    parts, spots_0 = laid(near[:3] + far[:1])
    sums_0 = windows(lists, module, z, parts, spots_0)
    parts, spots_1 = laid(near[3:] + far[1:3])
    sums_1 = windows(lists, module, z, parts, spots_1)
    parts, spots_2 = laid(far[3:])
    dealt = windows(lists, module, z, parts, spots_2, (spots_0, spots_1), (sums_0, sums_1))

    arrived = lax.all_to_all(dealt, ("x", "y"), 0, 0, tiled=True).sum(axis=0)
    arrived = arrived.reshape(2, SLOT, MODULES)[:, :ROWS]
    z_hi = lax.axis_index("z_hi")
    first = lax.ppermute(lax.dynamic_index_in_dim(arrived, z_hi, 0, False), ALL_AXES, home(0))
    second = lax.ppermute(lax.dynamic_index_in_dim(arrived, 1 - z_hi, 0, False), ALL_AXES, home(1))
    return jnp.log1p(first + second)


def home(flip):
    pairs = []
    for c in range(COHORTS):
        for x in range(4):
            for y in range(4):
                for z_hi in range(2):
                    slot = z_hi ^ flip
                    there = (2 * y + slot - c) % COHORTS
                    pairs.append((c * 32 + (x * 4 + y) * 2 + z_hi, there * 32 + (x * 4 + y) * 2 + slot))
    return pairs


def solution(mesh):
    finer = Mesh(mesh.devices.reshape(4, 2, 4, 4, 2), ALL_AXES)
    placed = (P(GENE_AXES, None), P(COHORT_AXES, None), P(GENE_AXES))
    return jax.shard_map(in_plane, mesh=finer, in_specs=placed, out_specs=P(ALL_AXES, None), check_vma=False)
```
